32 devices in a mesh: rows: 4 (over z), cols: 2 (over x), slabs: 4 (over y, core).
Axes of the slice: x: 2, y: 2, z: 4, core: 2. Of those that a mesh axis runs over, the one named last changes fastest.
Arguments:
- pressure: float32 [512, 8, 128, 128], P('rows', 'cols', 'slabs'), may hold values from 0.5 to 2
- earlier: float32 [512, 8, 128, 128], P('rows', 'cols', 'slabs'), may hold values from 0.2 to 1.8
- speed_square: float32 [512, 8, 128, 128], P('rows', 'cols', 'slabs'), may hold values from 0.05 to 0.3
Outputs:
- scaled_field: float32 [512, 8, 128, 128], P('rows', 'cols', 'slabs')
- pressure_end: float32 [512, 8, 128, 128], P('rows', 'cols', 'slabs')
The draws below stay inside these ranges and needn't reach their ends.
All inputs are finite; a program needn't handle non-finite values.
Results may differ from the reference program's by a relative error of at most 0.00002.
Values sent between devices are 32-bit elements; how exact they have to be, the bound alone decides.
A program may use at most 128 MiB of HBM per device.

```python
import jax
import jax.numpy as jnp
from jax import lax

GRID_J = 512
GRID_I = 8
GRID_K = 128
MEMBERS = 128
STEPS = 3


def block_scale(key, extent, pieces, least, top_value):
    loudness, own = 1.0, jax.random.fold_in(key, 6)
    for position, blocks in pieces:
        heights = jnp.exp(jax.random.uniform(jax.random.fold_in(own, position), (blocks,), jnp.float32, least / len(pieces), top_value / len(pieces)))
        loudness = loudness * jnp.repeat(heights, extent[position] // blocks).reshape([-1 if axis == position else 1 for axis in range(len(extent))])
    return loudness


def setup_inputs(seed: int = 0) -> dict:
    streams_of = jax.random.split(jax.random.key(seed), 4)
    pressure = jnp.clip(0.5 + 1.5 * jax.random.uniform(streams_of[0], (GRID_J, GRID_I, GRID_K, MEMBERS), jnp.float32) ** block_scale(streams_of[0], (GRID_J, GRID_I, GRID_K, MEMBERS), ((0, 4), (1, 2), (2, 4)), -0.2, 0.2), 0.5, 2.0)
    earlier = jnp.clip(0.2 + 1.5999999 * jax.random.uniform(streams_of[1], (GRID_J, GRID_I, GRID_K, MEMBERS), jnp.float32) ** block_scale(streams_of[1], (GRID_J, GRID_I, GRID_K, MEMBERS), ((0, 4), (1, 2), (2, 4)), -0.2, 0.2), 0.2, 1.8)
    speed_square = jnp.clip(0.05 + 0.25 * jax.random.uniform(streams_of[2], (GRID_J, GRID_I, GRID_K, MEMBERS), jnp.float32) ** block_scale(streams_of[2], (GRID_J, GRID_I, GRID_K, MEMBERS), ((0, 4), (1, 2), (2, 4)), -0.2, 0.2), 0.05, 0.3)
    return dict(pressure=pressure, earlier=earlier, speed_square=speed_square)


def strip_edges(values, dims):
    for dim in dims:
        values = lax.slice_in_dim(values, 1, values.shape[dim] - 1, axis=dim)
    return values

def neighbour(values, dim, start, dims):
    others = [other for other in dims if other != dim]
    values = strip_edges(values, others)
    return lax.slice_in_dim(values, start, start + values.shape[dim] - 2, axis=dim)

def one_step(padded, before, speed_square):
    middle = strip_edges(padded, (0, 1, 2))
    lower = [neighbour(padded, dim, 0, (0, 1, 2)) for dim in (0, 1, 2)]
    upper = [neighbour(padded, dim, 2, (0, 1, 2)) for dim in (0, 1, 2)]
    spread = lower[0] + upper[0] + lower[1] + upper[1] + lower[2] + upper[2] - 6.0 * middle
    return 2.0 * middle - before + speed_square * spread

def reference(pressure, earlier, speed_square):
    for step in range(STEPS):
        later = one_step(jnp.pad(pressure, ((1, 1), (1, 1), (1, 1), (0, 0)), mode='wrap'), earlier, speed_square)
        earlier, pressure = (pressure, later)
    line_mean = lax.optimization_barrier(jnp.mean(pressure, axis=0, keepdims=True))
    centred = pressure - line_mean
    line_variance = lax.optimization_barrier(jnp.mean(centred * centred, axis=0, keepdims=True))
    scaled_field = centred * lax.rsqrt(line_variance + 0.0001)
    return (scaled_field, pressure)
```

```python
import functools

import jax
import jax.numpy as jnp
from jax import lax
from jax.experimental import pallas as pl
from jax.experimental.pallas import tpu as pltpu
from jax.sharding import PartitionSpec as P

STEPS = 3
GUESS = 1.0
EPS = 0.0001
MESH = pl.DeviceIdType.MESH
TILE = 8
PIECES = 4
LO, HI = 0, 1


def leapfrog(sizes, p_hbm, e_hbm, s_hbm, end, stat,
             even, odd, xh, yh, line,
             xs, xr, ps, pr, ys, yr, zs, zr, ls, lr, own):
    speed = end
    rows, cols, slabs = sizes
    planes, cells, depth = p_hbm.shape[0], p_hbm.shape[1], p_hbm.shape[2]
    tiles = depth // TILE
    body_planes = pl.ds(1, planes)
    row, col, slab = (lax.axis_index(name) for name in ("rows", "cols", "slabs"))

    def shifted(name, index, count, by):
        return {name: lax.rem(index + by + count, count)}

    x_to = (shifted("cols", col, cols, -1), shifted("cols", col, cols, 1))
    y_to = (shifted("slabs", slab, slabs, -1), shifted("slabs", slab, slabs, 1))
    z_to = (shifted("rows", row, rows, -1), shifted("rows", row, rows, 1))
    peers = [shifted("rows", row, rows, d) for d in range(1, rows)]

    loads = [
        pltpu.make_async_copy(p_hbm, even.at[body_planes], own.at[0]),
        pltpu.make_async_copy(e_hbm, odd.at[body_planes], own.at[1]),
        pltpu.make_async_copy(s_hbm, speed, own.at[2]),
    ]
    barrier = pltpu.get_barrier_semaphore()
    greeted = list(x_to) + list(y_to) + peers
    for device in greeted:
        pl.semaphore_signal(barrier, inc=1, device_id=device, device_id_type=MESH)
    pl.semaphore_wait(barrier, len(greeted))

    fields = (even, odd)
    count = float(planes * rows)

    def line_copies(cell, q):
        part = line.at[row, cell, q]
        return [remote(part, part, ls.at[cell, q, d], lr.at[cell, q, d], device)
                for d, device in enumerate(peers)]

    def remote(src, dst, send, recv, device):
        return pltpu.make_async_remote_copy(
            src_ref=src, dst_ref=dst, send_sem=send, recv_sem=recv,
            device_id=device, device_id_type=MESH,
        )

    def source(step):
        return p_hbm if step == 0 else fields[step % 2].at[body_planes]

    def x_copy(step, side, q):
        cell = 0 if side == LO else cells - 1
        part = pl.ds(q * TILE, TILE)
        return remote(source(step).at[:, cell, part, :], xh.at[step, 1 - side, :, part, :],
                      xs.at[step, side, q], xr.at[step, side, q], x_to[side])

    def x_piece(side, piece):
        cell = 0 if side == LO else cells - 1
        q = tiles - 1
        here, part = pl.ds(piece * (planes // PIECES), planes // PIECES), pl.ds(q * TILE, TILE)
        return remote(source(STEPS - 1).at[here, cell, part, :], xh.at[STEPS - 1, 1 - side, here, part, :],
                      ps.at[piece], pr.at[piece], x_to[side])

    def x_copies(step, side, q):
        if step == STEPS - 1 and side == order(step)[1] and q == tiles - 1:
            return [x_piece(side, piece) for piece in range(PIECES)]
        return [x_copy(step, side, q)]

    def y_copy(step, side):
        part = pl.ds(0 if side == LO else depth - TILE, TILE)
        return remote(source(step).at[:, :, part, :], yh.at[step, 1 - side],
                      ys.at[step, side], yr.at[step, side], y_to[side])

    def z_copy(step, side):
        src = p_hbm.at[0 if side == LO else planes - 1] if step == 0 else (
            fields[step % 2].at[1 if side == LO else planes])
        dst = fields[step % 2].at[planes + 1 if side == LO else 0]
        return remote(src, dst, zs.at[step, side], zr.at[step, side], z_to[side])

    def order(step):
        return (LO, HI) if step % 2 == 0 else (HI, LO)

    def update(step, cell, q, low, high, copies=()):
        now, then = fields[step % 2], fields[(step + 1) % 2]
        part = pl.ds(q * TILE, TILE)
        index = lax.broadcasted_iota(jnp.int32, (TILE, TILE, 128), 1)
        last = step == STEPS - 1

        def block(b, sums):
            j = b * TILE
            here, padded = pl.ds(j, TILE), pl.ds(j + 1, TILE)
            mid = now[padded, cell, part, :]
            if q == 0:
                below = yh[step, LO, here, cell, TILE - 1:TILE, :]
            else:
                below = now[padded, cell, q * TILE - 1:q * TILE, :]
            if q == tiles - 1:
                above = yh[step, HI, here, cell, 0:1, :]
            else:
                above = now[padded, cell, (q + 1) * TILE:(q + 1) * TILE + 1, :]
            k_low = jnp.where(index == 0, below, pltpu.roll(mid, 1, 1))
            k_high = jnp.where(index == TILE - 1, above, pltpu.roll(mid, TILE - 1, 1))
            spread = (now[here, cell, part, :] + now[pl.ds(j + 2, TILE), cell, part, :]
                      + low(here, padded, part) + high(here, padded, part)
                      + k_low + k_high - 6.0 * mid)
            new = 2.0 * mid - then[padded, cell, part, :] + speed[here, cell, part, :] * spread
            if last:
                end[here, cell, part, :] = new
                moved = new - GUESS
                return sums[0] + jnp.sum(moved, axis=0), sums[1] + jnp.sum(moved * moved, axis=0)
            then[padded, cell, part, :] = new
            return sums

        zero = jnp.zeros((TILE, 128), jnp.float32)
        sums = (zero, zero) if last else 0
        count_of = max(len(copies), 1)
        blocks = planes // TILE // count_of
        for i in range(count_of):
            if copies:
                copies[i].wait_recv()
            sums = lax.fori_loop(i * blocks, (i + 1) * blocks, block, sums)
        if last:
            line[row, cell, q, 0] = sums[0]
            line[row, cell, q, 1] = sums[1]
            for copy in line_copies(cell, q):
                copy.start()

    def edge(step, side, q, copies):
        now = fields[step % 2]
        halo = lambda here, padded, part: xh[step, side, here, part, :]
        if side == LO:
            update(step, 0, q, halo, lambda here, padded, part: now[padded, 1, part, :], copies)
        else:
            update(step, cells - 1, q, lambda here, padded, part: now[padded, cells - 2, part, :], halo, copies)

    def edge_cell(side):
        return 0 if side == LO else cells - 1

    def interior(step):
        now = fields[step % 2]

        def at(cell, carry):
            for q in range(tiles):
                update(step, cell, q,
                       lambda here, padded, part: now[padded, cell - 1, part, :],
                       lambda here, padded, part: now[padded, cell + 1, part, :])
            return carry

        lax.fori_loop(1, cells - 1, at, 0)

    def settle(cell, parts):
        for q in parts:
            for copy in line_copies(cell, q):
                copy.wait()
            total, square = line[0, cell, q, 0], line[0, cell, q, 1]
            for r in range(1, rows):
                total, square = total + line[r, cell, q, 0], square + line[r, cell, q, 1]
            shift = total / count
            part = pl.ds(q * TILE, TILE)
            stat[0, cell, part, :] = GUESS + shift
            stat[1, cell, part, :] = lax.rsqrt(square / count - shift * shift + EPS)

    for side in order(0):
        for q in range(tiles):
            for copy in x_copies(0, side, q):
                copy.start()
    for side in (LO, HI):
        z_copy(0, side).start()
        y_copy(0, side).start()
    for load in loads:
        load.start()
    for load in loads:
        load.wait()

    for step in range(STEPS):
        if step >= 1:
            for side in order(step - 1):
                z_copy(step - 1, side).wait_send()
                y_copy(step - 1, side).wait_send()
                for q in range(tiles):
                    for copy in x_copies(step - 1, side, q):
                        copy.wait_send()
        for side in (LO, HI):
            z_copy(step, side).wait_recv()
            y_copy(step, side).wait_recv()
        interior(step)
        first, second = order(step)
        for side in (first, second):
            for q in range(tiles):
                edge(step, 1 - side, q, x_copies(step, side, q))
                if step < STEPS - 1:
                    for copy in x_copies(step + 1, 1 - side, q):
                        copy.start()
                elif side == first and q == 0:
                    for cell in range(1, cells - 1):
                        settle(cell, range(tiles))
                elif side == first:
                    settle(edge_cell(1 - first), [q - 1])
                elif q == 0:
                    settle(edge_cell(1 - first), [tiles - 1])
                else:
                    settle(edge_cell(1 - second), [q - 1])
        if step < STEPS - 1:
            for side in (LO, HI):
                z_copy(step + 1, side).start()
                y_copy(step + 1, side).start()

    for side in order(STEPS - 1):
        z_copy(STEPS - 1, side).wait_send()
        y_copy(STEPS - 1, side).wait_send()
        for q in range(tiles):
            for copy in x_copies(STEPS - 1, side, q):
                copy.wait_send()

    settle(edge_cell(1 - order(STEPS - 1)[1]), [tiles - 1])


def rescale(p_ref, stat_ref, scaled_hbm, end_hbm, scaled, end_sem, scaled_sem):
    planes, parts = p_ref.shape[0], end_sem.shape[0]
    each = planes // parts
    copies = []
    for c in range(parts):
        part = pl.ds(c * each, each)
        copies.append((pltpu.make_async_copy(p_ref.at[part], end_hbm.at[part], end_sem.at[c]),
                       pltpu.make_async_copy(scaled.at[part], scaled_hbm.at[part], scaled_sem.at[c])))

    for c in range(parts):
        copies[c][0].start()

        def plane(j, carry):
            scaled[j] = (p_ref[j] - stat_ref[0]) * stat_ref[1]
            return carry

        lax.fori_loop(c * each, (c + 1) * each, plane, 0, unroll=2)
        copies[c][1].start()
    for pair in copies:
        for copy in pair:
            copy.wait()


def shards(sizes, pressure, earlier, speed_square):
    rows = sizes[0]
    planes, cells, depth, members = pressure.shape
    tiles = depth // TILE
    any_space = pl.BlockSpec(memory_space=pl.ANY)
    dma = pltpu.SemaphoreType.DMA
    vmem_space = pl.BlockSpec(memory_space=pltpu.VMEM)
    end, stat = pl.pallas_call(
        functools.partial(leapfrog, sizes),
        out_shape=(
            pltpu.VMEM(pressure.shape, jnp.float32),
            pltpu.VMEM((2, cells, depth, members), jnp.float32),
        ),
        in_specs=[any_space] * 3,
        out_specs=(vmem_space, vmem_space),
        scratch_shapes=[
            pltpu.VMEM((planes + 2, cells, depth, members), jnp.float32),
            pltpu.VMEM((planes + 2, cells, depth, members), jnp.float32),
            pltpu.VMEM((STEPS, 2, planes, depth, members), jnp.float32),
            pltpu.VMEM((STEPS, 2, planes, cells, TILE, members), jnp.float32),
            pltpu.VMEM((rows, cells, tiles, 2, TILE, members), jnp.float32),
            dma((STEPS, 2, tiles)), dma((STEPS, 2, tiles)), dma((PIECES,)), dma((PIECES,)),
            dma((STEPS, 2)), dma((STEPS, 2)),
            dma((STEPS, 2)), dma((STEPS, 2)),
            dma((cells, tiles, rows - 1)), dma((cells, tiles, rows - 1)),
            dma((3,)),
        ],
        compiler_params=pltpu.CompilerParams(
            collective_id=0, has_side_effects=True, vmem_limit_bytes=46 * 1024 * 1024
        ),
    )(pressure, earlier, speed_square)

    parts = 8
    return pl.pallas_call(
        rescale,
        out_shape=(jax.ShapeDtypeStruct(pressure.shape, jnp.float32),) * 2,
        in_specs=[vmem_space, vmem_space],
        out_specs=(any_space, any_space),
        scratch_shapes=[pltpu.VMEM(pressure.shape, jnp.float32), dma((parts,)), dma((parts,))],
        compiler_params=pltpu.CompilerParams(vmem_limit_bytes=24 * 1024 * 1024),
    )(end, stat)


def solution(mesh):
    spec = P("rows", "cols", "slabs", None)
    sizes = tuple(mesh.shape[name] for name in ("rows", "cols", "slabs"))
    return jax.shard_map(functools.partial(shards, sizes), mesh=mesh,
                         in_specs=(spec,) * 3, out_specs=(spec,) * 2, check_vma=False)
```

```python
import functools

import jax
import jax.numpy as jnp
from jax import lax
from jax.experimental import pallas as pl
from jax.experimental.pallas import tpu as pltpu
from jax.sharding import PartitionSpec as P

STEPS = 3
GUESS = 1.0
EPS = 0.0001
MESH = pl.DeviceIdType.MESH
TILE = 8
PIECES = 4
PARTS = 8
LO, HI = 0, 1


def leapfrog(sizes, p_hbm, e_hbm, s_hbm, end, stat,
             even, odd, xh, yh, line,
             xs, xr, xp, ys, yr, zs, zr, ls, lr, own):
    speed = end
    rows, cols, slabs = sizes
    planes, cells, depth = p_hbm.shape[0], p_hbm.shape[1], p_hbm.shape[2]
    tiles = depth // TILE
    body_planes = pl.ds(1, planes)
    row, col, slab = (lax.axis_index(name) for name in ("rows", "cols", "slabs"))

    def shifted(name, index, count, by):
        return {name: lax.rem(index + by + count, count)}

    x_to = (shifted("cols", col, cols, -1), shifted("cols", col, cols, 1))
    y_to = (shifted("slabs", slab, slabs, -1), shifted("slabs", slab, slabs, 1))
    z_to = (shifted("rows", row, rows, -1), shifted("rows", row, rows, 1))
    peers = [shifted("rows", row, rows, d) for d in range(1, rows)]

    loads = [
        pltpu.make_async_copy(p_hbm, even.at[body_planes], own.at[0]),
        pltpu.make_async_copy(e_hbm, odd.at[body_planes], own.at[1]),
        pltpu.make_async_copy(s_hbm, speed, own.at[2]),
    ]
    barrier = pltpu.get_barrier_semaphore()
    near = y_to + z_to

    def greet(devices):
        for device in devices:
            pl.semaphore_signal(barrier, inc=1, device_id=device, device_id_type=MESH)

    colored = rows % 2 == 0 and slabs % 2 == 0
    color = lax.rem(row + slab, 2)
    greet(x_to)
    if colored:
        pl.semaphore_wait(barrier, len(x_to) + len(near) * color)
        greet(near)
    else:
        greet(near)
        pl.semaphore_wait(barrier, len(x_to) + len(near))

    fields = (even, odd)
    count = float(planes * rows)

    def order(step):
        return (LO, HI) if step % 2 == 0 else (HI, LO)

    def edge_cell(side):
        return 0 if side == LO else cells - 1

    early, late = (edge_cell(1 - side) for side in order(STEPS - 1))
    groups = [
        (pl.ds(1, cells - 2), slice(None), [(c, q) for c in range(1, cells - 1) for q in range(tiles)]),
        (early, slice(None), [(early, q) for q in range(tiles)]),
        (late, pl.ds(0, tiles - 1), [(late, q) for q in range(tiles - 1)]),
        (late, tiles - 1, [(late, tiles - 1)]),
    ]

    def line_copy(group, d):
        part = line.at[row, groups[group][0], groups[group][1]]
        return remote(part, part, ls.at[d], lr.at[group, d], peers[d])

    def send_lines(group):
        for d in range(rows - 1):
            if group > 0:
                line_copy(group - 1, d).wait_send()
            line_copy(group, d).start()

    def remote(src, dst, send, recv, device):
        return pltpu.make_async_remote_copy(
            src_ref=src, dst_ref=dst, send_sem=send, recv_sem=recv,
            device_id=device, device_id_type=MESH,
        )

    def source(step):
        return p_hbm if step == 0 else fields[step % 2].at[body_planes]

    def x_part(step, side, here, part, recv):
        return remote(source(step).at[here, edge_cell(side), part, :], xh.at[step, 1 - side, here, part, :],
                      xs.at[step % 2, side], recv, x_to[side])

    def x_copies(step, side, q):
        part = pl.ds(q * TILE, TILE)
        if step == STEPS - 1 and side == order(step)[1] and q == tiles - 1:
            each = planes // PIECES
            return [x_part(step, side, pl.ds(piece * each, each), part, xp.at[piece]) for piece in range(PIECES)]
        return [x_part(step, side, slice(None), part, xr.at[step % 2, side, q])]

    def x_sent(step, side):
        x_part(step, side, slice(None), slice(None), xp.at[0]).wait_send()

    def y_copy(step, side):
        part = pl.ds(0 if side == LO else depth - TILE, TILE)
        return remote(source(step).at[:, :, part, :], yh.at[step, 1 - side],
                      ys.at[step % 2, side], yr.at[step % 2, side], y_to[side])

    def z_copy(step, side):
        src = p_hbm.at[0 if side == LO else planes - 1] if step == 0 else (
            fields[step % 2].at[1 if side == LO else planes])
        dst = fields[step % 2].at[planes + 1 if side == LO else 0]
        return remote(src, dst, zs.at[step % 2, side], zr.at[step % 2, side], z_to[side])

    def update(step, cell, q, low, high, copies=(), before_last=None):
        now, then = fields[step % 2], fields[(step + 1) % 2]
        part = pl.ds(q * TILE, TILE)
        index = lax.broadcasted_iota(jnp.int32, (TILE, TILE, 128), 1)
        last = step == STEPS - 1

        def block(b, sums):
            j = b * TILE
            here, padded = pl.ds(j, TILE), pl.ds(j + 1, TILE)
            mid = now[padded, cell, part, :]
            if q == 0:
                below = yh[step, LO, here, cell, TILE - 1:TILE, :]
            else:
                below = now[padded, cell, q * TILE - 1:q * TILE, :]
            if q == tiles - 1:
                above = yh[step, HI, here, cell, 0:1, :]
            else:
                above = now[padded, cell, (q + 1) * TILE:(q + 1) * TILE + 1, :]
            k_low = jnp.where(index == 0, below, pltpu.roll(mid, 1, 1))
            k_high = jnp.where(index == TILE - 1, above, pltpu.roll(mid, TILE - 1, 1))
            spread = (now[here, cell, part, :] + now[pl.ds(j + 2, TILE), cell, part, :]
                      + low(here, padded, part) + high(here, padded, part)
                      + k_low + k_high - 6.0 * mid)
            new = 2.0 * mid - then[padded, cell, part, :] + speed[here, cell, part, :] * spread
            if last:
                end[here, cell, part, :] = new
                moved = new - GUESS
                return sums[0] + jnp.sum(moved, axis=0), sums[1] + jnp.sum(moved * moved, axis=0)
            then[padded, cell, part, :] = new
            return sums

        zero = jnp.zeros((TILE, 128), jnp.float32)
        sums = (zero, zero) if last else 0
        count_of = max(len(copies), 1)
        blocks = planes // TILE // count_of
        for i in range(count_of):
            if before_last is not None and i == count_of - 1:
                before_last()
            if copies:
                copies[i].wait_recv()
            sums = lax.fori_loop(i * blocks, (i + 1) * blocks, block, sums)
        if last:
            line[row, cell, q, 0] = sums[0]
            line[row, cell, q, 1] = sums[1]

    def edge(step, side, q, copies, before_last):
        now = fields[step % 2]
        halo = lambda here, padded, part: xh[step, side, here, part, :]
        if side == LO:
            update(step, 0, q, halo, lambda here, padded, part: now[padded, 1, part, :], copies, before_last)
        else:
            update(step, cells - 1, q, lambda here, padded, part: now[padded, cells - 2, part, :], halo, copies, before_last)

    def interior(step):
        now = fields[step % 2]

        def at(cell, carry):
            for q in range(tiles):
                update(step, cell, q,
                       lambda here, padded, part: now[padded, cell - 1, part, :],
                       lambda here, padded, part: now[padded, cell + 1, part, :])
            return carry

        lax.fori_loop(1, cells - 1, at, 0)

    def settle(group):
        for d in range(rows - 1):
            line_copy(group, d).wait_recv()
        for cell, q in groups[group][2]:
            total, square = line[0, cell, q, 0], line[0, cell, q, 1]
            for r in range(1, rows):
                total, square = total + line[r, cell, q, 0], square + line[r, cell, q, 1]
            shift = total / count
            part = pl.ds(q * TILE, TILE)
            stat[0, cell, part, :] = GUESS + shift
            stat[1, cell, part, :] = lax.rsqrt(square / count - shift * shift + EPS)

    for side in order(0):
        for q in range(tiles):
            for copy in x_copies(0, side, q):
                copy.start()
    if colored:
        @pl.when(color == 0)
        def _():
            pl.semaphore_wait(barrier, len(near))

    for side in (LO, HI):
        z_copy(0, side).start()
        y_copy(0, side).start()
    for load in loads:
        load.start()
    for load in loads:
        load.wait()

    for step in range(STEPS):
        if step >= 1:
            for side in order(step - 1):
                z_copy(step - 1, side).wait_send()
                y_copy(step - 1, side).wait_send()
                x_sent(step - 1, side)
        for side in (LO, HI):
            z_copy(step, side).wait_recv()
            y_copy(step, side).wait_recv()
        interior(step)
        if step == STEPS - 1:
            send_lines(0)
        first, second = order(step)
        for side in (first, second):
            for q in range(tiles):
                final = step == STEPS - 1
                hook = functools.partial(settle, 2) if final and side == second and q == tiles - 1 else None
                edge(step, 1 - side, q, x_copies(step, side, q), hook)
                if not final:
                    for copy in x_copies(step + 1, 1 - side, q):
                        copy.start()
                elif side == first:
                    if q == 0:
                        settle(0)
                    if q == tiles - 1:
                        send_lines(1)
                else:
                    if q == 0:
                        settle(1)
                    if q >= tiles - 2:
                        send_lines(q - tiles + 4)
        if step < STEPS - 1:
            for side in (LO, HI):
                z_copy(step + 1, side).start()
                y_copy(step + 1, side).start()

    for side in order(STEPS - 1):
        z_copy(STEPS - 1, side).wait_send()
        y_copy(STEPS - 1, side).wait_send()
        x_sent(STEPS - 1, side)

    settle(3)
    for d in range(rows - 1):
        line_copy(3, d).wait_send()


def rescale(p_ref, stat_ref, scaled_hbm, end_hbm, scaled, end_sem, scaled_sem):
    planes = p_ref.shape[0]
    each = planes // PARTS
    parts = [pl.ds(c * each, each) for c in range(PARTS)]
    for part in parts:
        pltpu.make_async_copy(p_ref.at[part], end_hbm.at[part], end_sem).start()

    def plane(j, carry):
        scaled[j] = (p_ref[j] - stat_ref[0]) * stat_ref[1]
        return carry

    for c, part in enumerate(parts):
        lax.fori_loop(c * each, (c + 1) * each, plane, 0, unroll=2)
        pltpu.make_async_copy(scaled.at[part], scaled_hbm.at[part], scaled_sem).start()
    pltpu.make_async_copy(p_ref, end_hbm, end_sem).wait()
    pltpu.make_async_copy(scaled, scaled_hbm, scaled_sem).wait()


def shards(sizes, pressure, earlier, speed_square):
    rows = sizes[0]
    planes, cells, depth, members = pressure.shape
    tiles = depth // TILE
    any_space = pl.BlockSpec(memory_space=pl.ANY)
    dma = pltpu.SemaphoreType.DMA
    vmem_space = pl.BlockSpec(memory_space=pltpu.VMEM)
    end, stat = pl.pallas_call(
        functools.partial(leapfrog, sizes),
        out_shape=(
            pltpu.VMEM(pressure.shape, jnp.float32),
            pltpu.VMEM((2, cells, depth, members), jnp.float32),
        ),
        in_specs=[any_space] * 3,
        out_specs=(vmem_space, vmem_space),
        scratch_shapes=[
            pltpu.VMEM((planes + 2, cells, depth, members), jnp.float32),
            pltpu.VMEM((planes + 2, cells, depth, members), jnp.float32),
            pltpu.VMEM((STEPS, 2, planes, depth, members), jnp.float32),
            pltpu.VMEM((STEPS, 2, planes, cells, TILE, members), jnp.float32),
            pltpu.VMEM((rows, cells, tiles, 2, TILE, members), jnp.float32),
            dma((2, 2)), dma((2, 2, tiles)), dma((PIECES,)),
            dma((2, 2)), dma((2, 2)),
            dma((2, 2)), dma((2, 2)),
            dma((rows - 1,)), dma((4, rows - 1)),
            dma((3,)),
        ],
        compiler_params=pltpu.CompilerParams(
            collective_id=0, has_side_effects=True, vmem_limit_bytes=46 * 1024 * 1024
        ),
    )(pressure, earlier, speed_square)

    return pl.pallas_call(
        rescale,
        out_shape=(jax.ShapeDtypeStruct(pressure.shape, jnp.float32),) * 2,
        in_specs=[vmem_space, vmem_space],
        out_specs=(any_space, any_space),
        scratch_shapes=[pltpu.VMEM(pressure.shape, jnp.float32), dma, dma],
        compiler_params=pltpu.CompilerParams(vmem_limit_bytes=24 * 1024 * 1024),
    )(end, stat)


def solution(mesh):
    spec = P("rows", "cols", "slabs", None)
    sizes = tuple(mesh.shape[name] for name in ("rows", "cols", "slabs"))
    return jax.shard_map(functools.partial(shards, sizes), mesh=mesh,
                         in_specs=(spec,) * 3, out_specs=(spec,) * 2, check_vma=False)
```

```python
import functools

import jax
import jax.numpy as jnp
from jax import lax
from jax.experimental import pallas as pl
from jax.experimental.pallas import tpu as pltpu
from jax.sharding import PartitionSpec as P

STEPS = 3
GUESS = 1.0
EPS = 0.0001
MESH = pl.DeviceIdType.MESH
TILE = 8
PIECES = 4
PARTS = 8
LO, HI = 0, 1


def leapfrog(sizes, p_hbm, e_hbm, s_hbm, end, stat,
             even, odd, xh, yh, line,
             xs, xr, xp, ys, yr, zs, zr, ls, lr, own, heard):
    speed = end
    rows, cols, slabs = sizes
    planes, cells, depth = p_hbm.shape[0], p_hbm.shape[1], p_hbm.shape[2]
    tiles = depth // TILE
    body_planes = pl.ds(1, planes)
    row, col, slab = (lax.axis_index(name) for name in ("rows", "cols", "slabs"))

    def shifted(name, index, count, by):
        return {name: lax.rem(index + by + count, count)}

    x_to = (shifted("cols", col, cols, -1), shifted("cols", col, cols, 1))
    y_to = (shifted("slabs", slab, slabs, -1), shifted("slabs", slab, slabs, 1))
    z_to = (shifted("rows", row, rows, -1), shifted("rows", row, rows, 1))
    peers = [shifted("rows", row, rows, d) for d in range(1, rows)]

    loads = [
        pltpu.make_async_copy(p_hbm, even.at[body_planes], own.at[0]),
        pltpu.make_async_copy(e_hbm, odd.at[body_planes], own.at[1]),
        pltpu.make_async_copy(s_hbm, speed, own.at[2]),
    ]
    barrier = pltpu.get_barrier_semaphore()
    near = y_to + z_to

    def greet(devices):
        for device in devices:
            pl.semaphore_signal(barrier, inc=1, device_id=device, device_id_type=MESH)

    paired = slabs % 2 == 0
    early = lax.rem(slab, 2) == 0
    greet(x_to)
    if paired:
        pl.when(jnp.logical_not(early))(lambda: greet(z_to))
        pl.semaphore_wait(barrier, len(x_to) + len(near) * lax.rem(slab, 2))
        greet(y_to)
    else:
        greet(near)
        pl.semaphore_wait(barrier, len(x_to) + len(near))

    fields = (even, odd)
    count = float(planes * rows)

    def order(step):
        return (LO, HI) if step % 2 == 0 else (HI, LO)

    def edge_cell(side):
        return 0 if side == LO else cells - 1

    sooner, later = (edge_cell(1 - side) for side in order(STEPS - 1))
    groups = [
        (pl.ds(1, cells - 2), slice(None), [(c, q) for c in range(1, cells - 1) for q in range(tiles)]),
        (sooner, slice(None), [(sooner, q) for q in range(tiles)]),
        (later, pl.ds(0, tiles - 1), [(later, q) for q in range(tiles - 1)]),
        (later, tiles - 1, [(later, tiles - 1)]),
    ]

    def line_copy(group, d):
        part = line.at[row, groups[group][0], groups[group][1]]
        return remote(part, part, ls.at[d], lr.at[group, d], peers[d])

    def send_lines(group):
        for d in range(rows - 1):
            if group > 0:
                line_copy(group - 1, d).wait_send()
            line_copy(group, d).start()

    def remote(src, dst, send, recv, device):
        return pltpu.make_async_remote_copy(
            src_ref=src, dst_ref=dst, send_sem=send, recv_sem=recv,
            device_id=device, device_id_type=MESH,
        )

    def source(step):
        return p_hbm if step == 0 else fields[step % 2].at[body_planes]

    def x_part(step, side, here, part, recv):
        return remote(source(step).at[here, edge_cell(side), part, :], xh.at[step, 1 - side, here, part, :],
                      xs.at[step % 2, side], recv, x_to[side])

    def x_copies(step, side, q):
        part = pl.ds(q * TILE, TILE)
        if step == STEPS - 1 and side == order(step)[1] and q == tiles - 1:
            each = planes // PIECES
            return [x_part(step, side, pl.ds(piece * each, each), part, xp.at[piece]) for piece in range(PIECES)]
        return [x_part(step, side, slice(None), part, xr.at[step % 2, side, q])]

    def x_sent(step, side):
        x_part(step, side, slice(None), slice(None), xp.at[0]).wait_send()

    def y_copy(step, side):
        part = pl.ds(0 if side == LO else depth - TILE, TILE)
        return remote(source(step).at[:, :, part, :], yh.at[step, 1 - side],
                      ys.at[side], yr.at[step % 2, side], y_to[side])

    def z_copy(step, side):
        src = p_hbm.at[0 if side == LO else planes - 1] if step == 0 else (
            fields[step % 2].at[1 if side == LO else planes])
        dst = fields[step % 2].at[planes + 1 if side == LO else 0]
        return remote(src, dst, zs.at[side], zr.at[step % 2, side], z_to[side])

    def update(step, cell, q, low, high, copies=(), before_last=None):
        now, then = fields[step % 2], fields[(step + 1) % 2]
        part = pl.ds(q * TILE, TILE)
        index = lax.broadcasted_iota(jnp.int32, (TILE, TILE, 128), 1)
        last = step == STEPS - 1

        def block(b, sums):
            j = b * TILE
            here, padded = pl.ds(j, TILE), pl.ds(j + 1, TILE)
            mid = now[padded, cell, part, :]
            if q == 0:
                below = yh[step, LO, here, cell, TILE - 1:TILE, :]
            else:
                below = now[padded, cell, q * TILE - 1:q * TILE, :]
            if q == tiles - 1:
                above = yh[step, HI, here, cell, 0:1, :]
            else:
                above = now[padded, cell, (q + 1) * TILE:(q + 1) * TILE + 1, :]
            k_low = jnp.where(index == 0, below, pltpu.roll(mid, 1, 1))
            k_high = jnp.where(index == TILE - 1, above, pltpu.roll(mid, TILE - 1, 1))
            spread = (now[here, cell, part, :] + now[pl.ds(j + 2, TILE), cell, part, :]
                      + low(here, padded, part) + high(here, padded, part)
                      + k_low + k_high - 6.0 * mid)
            new = 2.0 * mid - then[padded, cell, part, :] + speed[here, cell, part, :] * spread
            if last:
                end[here, cell, part, :] = new
                moved = new - GUESS
                return sums[0] + jnp.sum(moved, axis=0), sums[1] + jnp.sum(moved * moved, axis=0)
            then[padded, cell, part, :] = new
            return sums

        zero = jnp.zeros((TILE, 128), jnp.float32)
        sums = (zero, zero) if last else 0
        count_of = max(len(copies), 1)
        blocks = planes // TILE // count_of
        for i in range(count_of):
            if before_last is not None and i == count_of - 1:
                before_last()
            if copies:
                copies[i].wait_recv()
            sums = lax.fori_loop(i * blocks, (i + 1) * blocks, block, sums)
        if last:
            line[row, cell, q, 0] = sums[0]
            line[row, cell, q, 1] = sums[1]

    def edge(step, side, q, copies, before_last):
        now = fields[step % 2]
        halo = lambda here, padded, part: xh[step, side, here, part, :]
        if side == LO:
            update(step, 0, q, halo, lambda here, padded, part: now[padded, 1, part, :], copies, before_last)
        else:
            update(step, cells - 1, q, lambda here, padded, part: now[padded, cells - 2, part, :], halo, copies, before_last)

    def interior(step):
        now = fields[step % 2]

        def at(cell, carry):
            for q in range(tiles):
                update(step, cell, q,
                       lambda here, padded, part: now[padded, cell - 1, part, :],
                       lambda here, padded, part: now[padded, cell + 1, part, :])
            return carry

        lax.fori_loop(1, cells - 1, at, 0)

    def settle(group):
        for d in range(rows - 1):
            line_copy(group, d).wait_recv()
        for cell, q in groups[group][2]:
            total, square = line[0, cell, q, 0], line[0, cell, q, 1]
            for r in range(1, rows):
                total, square = total + line[r, cell, q, 0], square + line[r, cell, q, 1]
            shift = total / count
            part = pl.ds(q * TILE, TILE)
            stat[0, cell, part, :] = GUESS + shift
            stat[1, cell, part, :] = lax.rsqrt(square / count - shift * shift + EPS)

    def start_cols():
        for side in order(0):
            for q in range(tiles):
                for copy in x_copies(0, side, q):
                    copy.start()

    if paired:
        pl.when(early)(start_cols)
    else:
        start_cols()
    def swap_rows():
        for side in (LO, HI):
            z_copy(0, side).start()
        for side in (LO, HI):
            z_copy(0, side).wait_recv()

    def start_early():
        pl.semaphore_wait(barrier, len(y_to))
        for side in (LO, HI):
            y_copy(0, side).start()
        pl.semaphore_wait(heard, len(y_to))
        swap_rows()

    def start_late():
        for side in (LO, HI):
            y_copy(0, side).start()
        swap_rows()
        for device in y_to:
            pl.semaphore_signal(heard, inc=1, device_id=device, device_id_type=MESH)

    for load in loads:
        load.start()
    if paired:
        pl.when(early)(start_early)
        pl.when(jnp.logical_not(early))(start_late)
    else:
        for side in (LO, HI):
            y_copy(0, side).start()
        swap_rows()
    for load in loads:
        load.wait()
    if paired:
        pl.when(jnp.logical_not(early))(start_cols)

    for step in range(STEPS):
        if step >= 1:
            for side in order(step - 1):
                z_copy(step - 1, side).wait_send()
                y_copy(step - 1, side).wait_send()
                x_sent(step - 1, side)
        for side in (LO, HI):
            if step >= 1:
                z_copy(step, side).wait_recv()
            y_copy(step, side).wait_recv()
        interior(step)
        if step == STEPS - 1:
            send_lines(0)
        first, second = order(step)
        for side in (first, second):
            for q in range(tiles):
                final = step == STEPS - 1
                hook = functools.partial(settle, 2) if final and side == second and q == tiles - 1 else None
                edge(step, 1 - side, q, x_copies(step, side, q), hook)
                if not final:
                    for copy in x_copies(step + 1, 1 - side, q):
                        copy.start()
                elif side == first:
                    if q == 0:
                        settle(0)
                    if q == tiles - 1:
                        send_lines(1)
                else:
                    if q == 0:
                        settle(1)
                    if q >= tiles - 2:
                        send_lines(q - tiles + 4)
        if step < STEPS - 1:
            for side in (LO, HI):
                z_copy(step + 1, side).start()
                y_copy(step + 1, side).start()

    for side in order(STEPS - 1):
        z_copy(STEPS - 1, side).wait_send()
        y_copy(STEPS - 1, side).wait_send()
        x_sent(STEPS - 1, side)

    settle(3)
    for d in range(rows - 1):
        line_copy(3, d).wait_send()


def rescale(p_ref, stat_ref, scaled_hbm, end_hbm, scaled, end_sem, scaled_sem):
    planes = p_ref.shape[0]
    each = planes // PARTS
    parts = [pl.ds(c * each, each) for c in range(PARTS)]
    for part in parts:
        pltpu.make_async_copy(p_ref.at[part], end_hbm.at[part], end_sem).start()

    def plane(j, carry):
        scaled[j] = (p_ref[j] - stat_ref[0]) * stat_ref[1]
        return carry

    for c, part in enumerate(parts):
        lax.fori_loop(c * each, (c + 1) * each, plane, 0, unroll=2)
        pltpu.make_async_copy(scaled.at[part], scaled_hbm.at[part], scaled_sem).start()
    pltpu.make_async_copy(p_ref, end_hbm, end_sem).wait()
    pltpu.make_async_copy(scaled, scaled_hbm, scaled_sem).wait()


def shards(sizes, pressure, earlier, speed_square):
    rows = sizes[0]
    planes, cells, depth, members = pressure.shape
    tiles = depth // TILE
    any_space = pl.BlockSpec(memory_space=pl.ANY)
    dma = pltpu.SemaphoreType.DMA
    vmem_space = pl.BlockSpec(memory_space=pltpu.VMEM)
    end, stat = pl.pallas_call(
        functools.partial(leapfrog, sizes),
        out_shape=(
            pltpu.VMEM(pressure.shape, jnp.float32),
            pltpu.VMEM((2, cells, depth, members), jnp.float32),
        ),
        in_specs=[any_space] * 3,
        out_specs=(vmem_space, vmem_space),
        scratch_shapes=[
            pltpu.VMEM((planes + 2, cells, depth, members), jnp.float32),
            pltpu.VMEM((planes + 2, cells, depth, members), jnp.float32),
            pltpu.VMEM((STEPS, 2, planes, depth, members), jnp.float32),
            pltpu.VMEM((STEPS, 2, planes, cells, TILE, members), jnp.float32),
            pltpu.VMEM((rows, cells, tiles, 2, TILE, members), jnp.float32),
            dma((2, 2)), dma((2, 2, tiles)), dma((PIECES,)),
            dma((2,)), dma((2, 2)),
            dma((2,)), dma((2, 2)),
            dma((rows - 1,)), dma((4, rows - 1)),
            dma((3,)),
            pltpu.SemaphoreType.REGULAR,
        ],
        compiler_params=pltpu.CompilerParams(
            collective_id=0, has_side_effects=True, vmem_limit_bytes=46 * 1024 * 1024
        ),
    )(pressure, earlier, speed_square)

    return pl.pallas_call(
        rescale,
        out_shape=(jax.ShapeDtypeStruct(pressure.shape, jnp.float32),) * 2,
        in_specs=[vmem_space, vmem_space],
        out_specs=(any_space, any_space),
        scratch_shapes=[pltpu.VMEM(pressure.shape, jnp.float32), dma, dma],
        compiler_params=pltpu.CompilerParams(vmem_limit_bytes=24 * 1024 * 1024),
    )(end, stat)


def solution(mesh):
    spec = P("rows", "cols", "slabs", None)
    sizes = tuple(mesh.shape[name] for name in ("rows", "cols", "slabs"))
    return jax.shard_map(functools.partial(shards, sizes), mesh=mesh,
                         in_specs=(spec,) * 3, out_specs=(spec,) * 2, check_vma=False)
```

```python
import functools

import jax
import jax.numpy as jnp
from jax import lax
from jax.experimental import pallas as pl
from jax.experimental.pallas import tpu as pltpu
from jax.sharding import PartitionSpec as P

STEPS = 3
GUESS = 1.0
EPS = 0.0001
MESH = pl.DeviceIdType.MESH
TILE = 8
PARTS = 8
LO, HI = 0, 1


def halving(planes):
    spans, start = [], 0
    while planes - start > TILE:
        size = (planes - start) // (2 * TILE) * TILE
        spans.append((start, size))
        start += size
    return spans + [(start, planes - start)]


def leapfrog(sizes, p_hbm, e_hbm, s_hbm, end, stat,
             even, odd, xh, yh, line,
             xs, xr, xp, ys, yr, zs, zr, ls, lr, own, heard):
    speed = end
    rows, cols, slabs = sizes
    planes, cells, depth = p_hbm.shape[0], p_hbm.shape[1], p_hbm.shape[2]
    tiles = depth // TILE
    body_planes = pl.ds(1, planes)
    row, col, slab = (lax.axis_index(name) for name in ("rows", "cols", "slabs"))

    def shifted(name, index, count, by):
        return {name: lax.rem(index + by + count, count)}

    x_to = (shifted("cols", col, cols, -1), shifted("cols", col, cols, 1))
    y_to = (shifted("slabs", slab, slabs, -1), shifted("slabs", slab, slabs, 1))
    z_to = (shifted("rows", row, rows, -1), shifted("rows", row, rows, 1))
    peers = [shifted("rows", row, rows, d) for d in range(1, rows)]

    loads = [
        pltpu.make_async_copy(p_hbm, even.at[body_planes], own.at[0]),
        pltpu.make_async_copy(e_hbm, odd.at[body_planes], own.at[1]),
        pltpu.make_async_copy(s_hbm, speed, own.at[2]),
    ]
    barrier = pltpu.get_barrier_semaphore()
    near = y_to + z_to

    def greet(devices):
        for device in devices:
            pl.semaphore_signal(barrier, inc=1, device_id=device, device_id_type=MESH)

    paired = slabs % 2 == 0
    early = lax.rem(slab, 2) == 0
    greet(x_to)
    if paired:
        pl.when(jnp.logical_not(early))(lambda: greet(z_to))
        pl.semaphore_wait(barrier, len(x_to) + len(near) * lax.rem(slab, 2))
        greet(y_to)
    else:
        greet(near)
        pl.semaphore_wait(barrier, len(x_to) + len(near))

    fields = (even, odd)
    count = float(planes * rows)

    def order(step):
        return (LO, HI) if step % 2 == 0 else (HI, LO)

    def edge_cell(side):
        return 0 if side == LO else cells - 1

    sooner, later = (edge_cell(1 - side) for side in order(STEPS - 1))
    groups = [
        (pl.ds(1, cells - 2), slice(None), [(c, q) for c in range(1, cells - 1) for q in range(tiles)]),
        (sooner, slice(None), [(sooner, q) for q in range(tiles)]),
        (later, pl.ds(0, tiles - 1), [(later, q) for q in range(tiles - 1)]),
        (later, tiles - 1, [(later, tiles - 1)]),
    ]

    def line_copy(group, d):
        part = line.at[row, groups[group][0], groups[group][1]]
        return remote(part, part, ls.at[d], lr.at[group, d], peers[d])

    def send_lines(group):
        for d in range(rows - 1):
            if group > 0:
                line_copy(group - 1, d).wait_send()
            line_copy(group, d).start()

    def remote(src, dst, send, recv, device):
        return pltpu.make_async_remote_copy(
            src_ref=src, dst_ref=dst, send_sem=send, recv_sem=recv,
            device_id=device, device_id_type=MESH,
        )

    def source(step):
        return p_hbm if step == 0 else fields[step % 2].at[body_planes]

    def x_part(step, side, here, part, recv):
        return remote(source(step).at[here, edge_cell(side), part, :], xh.at[step, 1 - side, here, part, :],
                      xs.at[step % 2, side], recv, x_to[side])

    def x_copies(step, side, q):
        part = pl.ds(q * TILE, TILE)
        if step == STEPS - 1 and side == order(step)[1] and q == tiles - 1:
            return [x_part(step, side, pl.ds(*span), part, xp.at[i]) for i, span in enumerate(halving(planes))]
        return [x_part(step, side, slice(None), part, xr.at[step % 2, side, q])]

    def x_sent(step, side):
        x_part(step, side, slice(None), slice(None), xp.at[0]).wait_send()

    def y_copy(step, side):
        part = pl.ds(0 if side == LO else depth - TILE, TILE)
        return remote(source(step).at[:, :, part, :], yh.at[step, 1 - side],
                      ys.at[side], yr.at[step % 2, side], y_to[side])

    def z_copy(step, side):
        src = p_hbm.at[0 if side == LO else planes - 1] if step == 0 else (
            fields[step % 2].at[1 if side == LO else planes])
        dst = fields[step % 2].at[planes + 1 if side == LO else 0]
        return remote(src, dst, zs.at[side], zr.at[step % 2, side], z_to[side])

    def update(step, cell, q, low, high, copies=(), before_last=None):
        now, then = fields[step % 2], fields[(step + 1) % 2]
        part = pl.ds(q * TILE, TILE)
        index = lax.broadcasted_iota(jnp.int32, (TILE, TILE, 128), 1)
        last = step == STEPS - 1

        def block(b, sums):
            j = b * TILE
            here, padded = pl.ds(j, TILE), pl.ds(j + 1, TILE)
            mid = now[padded, cell, part, :]
            if q == 0:
                below = yh[step, LO, here, cell, TILE - 1:TILE, :]
            else:
                below = now[padded, cell, q * TILE - 1:q * TILE, :]
            if q == tiles - 1:
                above = yh[step, HI, here, cell, 0:1, :]
            else:
                above = now[padded, cell, (q + 1) * TILE:(q + 1) * TILE + 1, :]
            k_low = jnp.where(index == 0, below, pltpu.roll(mid, 1, 1))
            k_high = jnp.where(index == TILE - 1, above, pltpu.roll(mid, TILE - 1, 1))
            spread = (now[here, cell, part, :] + now[pl.ds(j + 2, TILE), cell, part, :]
                      + low(here, padded, part) + high(here, padded, part)
                      + k_low + k_high - 6.0 * mid)
            new = 2.0 * mid - then[padded, cell, part, :] + speed[here, cell, part, :] * spread
            if last:
                end[here, cell, part, :] = new
                moved = new - GUESS
                return sums[0] + jnp.sum(moved, axis=0), sums[1] + jnp.sum(moved * moved, axis=0)
            then[padded, cell, part, :] = new
            return sums

        zero = jnp.zeros((TILE, 128), jnp.float32)
        sums = (zero, zero) if last else 0
        spans = halving(planes) if len(copies) > 1 else [(0, planes)]
        for i, (start, size) in enumerate(spans):
            if before_last is not None and i == len(spans) - 1:
                before_last()
            if copies:
                copies[i].wait_recv()
            sums = lax.fori_loop(start // TILE, (start + size) // TILE, block, sums)
        if last:
            line[row, cell, q, 0] = sums[0]
            line[row, cell, q, 1] = sums[1]

    def edge(step, side, q, copies, before_last):
        now = fields[step % 2]
        halo = lambda here, padded, part: xh[step, side, here, part, :]
        if side == LO:
            update(step, 0, q, halo, lambda here, padded, part: now[padded, 1, part, :], copies, before_last)
        else:
            update(step, cells - 1, q, lambda here, padded, part: now[padded, cells - 2, part, :], halo, copies, before_last)

    def interior(step):
        now = fields[step % 2]

        def at(cell, carry):
            for q in range(tiles):
                update(step, cell, q,
                       lambda here, padded, part: now[padded, cell - 1, part, :],
                       lambda here, padded, part: now[padded, cell + 1, part, :])
            return carry

        lax.fori_loop(1, cells - 1, at, 0)

    def settle(group):
        for d in range(rows - 1):
            line_copy(group, d).wait_recv()
        for cell, q in groups[group][2]:
            total, square = line[0, cell, q, 0], line[0, cell, q, 1]
            for r in range(1, rows):
                total, square = total + line[r, cell, q, 0], square + line[r, cell, q, 1]
            shift = total / count
            part = pl.ds(q * TILE, TILE)
            stat[0, cell, part, :] = GUESS + shift
            stat[1, cell, part, :] = lax.rsqrt(square / count - shift * shift + EPS)

    def start_cols():
        for side in order(0):
            for q in range(tiles):
                for copy in x_copies(0, side, q):
                    copy.start()

    if paired:
        pl.when(early)(start_cols)
    else:
        start_cols()
    def swap_rows():
        for side in (LO, HI):
            z_copy(0, side).start()
        for side in (LO, HI):
            z_copy(0, side).wait_recv()

    def start_early():
        pl.semaphore_wait(barrier, len(y_to))
        for side in (LO, HI):
            y_copy(0, side).start()
        pl.semaphore_wait(heard, len(y_to))
        swap_rows()

    def start_late():
        for side in (LO, HI):
            y_copy(0, side).start()
        swap_rows()
        for device in y_to:
            pl.semaphore_signal(heard, inc=1, device_id=device, device_id_type=MESH)

    for load in loads:
        load.start()
    if paired:
        pl.when(early)(start_early)
        pl.when(jnp.logical_not(early))(start_late)
    else:
        for side in (LO, HI):
            y_copy(0, side).start()
        swap_rows()
    for load in loads:
        load.wait()
    if paired:
        pl.when(jnp.logical_not(early))(start_cols)

    for step in range(STEPS):
        if step >= 1:
            for side in order(step - 1):
                z_copy(step - 1, side).wait_send()
                y_copy(step - 1, side).wait_send()
                x_sent(step - 1, side)
        for side in (LO, HI):
            if step >= 1:
                z_copy(step, side).wait_recv()
            y_copy(step, side).wait_recv()
        interior(step)
        if step == STEPS - 1:
            send_lines(0)
        first, second = order(step)
        for side in (first, second):
            for q in range(tiles):
                final = step == STEPS - 1
                hook = functools.partial(settle, 2) if final and side == second and q == tiles - 1 else None
                edge(step, 1 - side, q, x_copies(step, side, q), hook)
                if not final:
                    for copy in x_copies(step + 1, 1 - side, q):
                        copy.start()
                elif side == first:
                    if q == 0:
                        settle(0)
                    if q == tiles - 1:
                        send_lines(1)
                else:
                    if q == 0:
                        settle(1)
                    if q >= tiles - 2:
                        send_lines(q - tiles + 4)
        if step < STEPS - 1:
            for side in (LO, HI):
                z_copy(step + 1, side).start()
                y_copy(step + 1, side).start()

    for side in order(STEPS - 1):
        z_copy(STEPS - 1, side).wait_send()
        y_copy(STEPS - 1, side).wait_send()
        x_sent(STEPS - 1, side)

    settle(3)
    for d in range(rows - 1):
        line_copy(3, d).wait_send()


def rescale(p_ref, stat_ref, scaled_hbm, end_hbm, scaled, end_sem, scaled_sem):
    planes = p_ref.shape[0]
    each = planes // PARTS
    parts = [pl.ds(c * each, each) for c in range(PARTS)]
    for part in parts:
        pltpu.make_async_copy(p_ref.at[part], end_hbm.at[part], end_sem).start()

    def plane(j, carry):
        scaled[j] = (p_ref[j] - stat_ref[0]) * stat_ref[1]
        return carry

    for c, part in enumerate(parts):
        lax.fori_loop(c * each, (c + 1) * each, plane, 0, unroll=2)
        pltpu.make_async_copy(scaled.at[part], scaled_hbm.at[part], scaled_sem).start()
    pltpu.make_async_copy(p_ref, end_hbm, end_sem).wait()
    pltpu.make_async_copy(scaled, scaled_hbm, scaled_sem).wait()


def shards(sizes, pressure, earlier, speed_square):
    rows = sizes[0]
    planes, cells, depth, members = pressure.shape
    tiles = depth // TILE
    any_space = pl.BlockSpec(memory_space=pl.ANY)
    dma = pltpu.SemaphoreType.DMA
    vmem_space = pl.BlockSpec(memory_space=pltpu.VMEM)
    end, stat = pl.pallas_call(
        functools.partial(leapfrog, sizes),
        out_shape=(
            pltpu.VMEM(pressure.shape, jnp.float32),
            pltpu.VMEM((2, cells, depth, members), jnp.float32),
        ),
        in_specs=[any_space] * 3,
        out_specs=(vmem_space, vmem_space),
        scratch_shapes=[
            pltpu.VMEM((planes + 2, cells, depth, members), jnp.float32),
            pltpu.VMEM((planes + 2, cells, depth, members), jnp.float32),
            pltpu.VMEM((STEPS, 2, planes, depth, members), jnp.float32),
            pltpu.VMEM((STEPS, 2, planes, cells, TILE, members), jnp.float32),
            pltpu.VMEM((rows, cells, tiles, 2, TILE, members), jnp.float32),
            dma((2, 2)), dma((2, 2, tiles)), dma((len(halving(planes)),)),
            dma((2,)), dma((2, 2)),
            dma((2,)), dma((2, 2)),
            dma((rows - 1,)), dma((4, rows - 1)),
            dma((3,)),
            pltpu.SemaphoreType.REGULAR,
        ],
        compiler_params=pltpu.CompilerParams(
            collective_id=0, has_side_effects=True, vmem_limit_bytes=46 * 1024 * 1024
        ),
    )(pressure, earlier, speed_square)

    return pl.pallas_call(
        rescale,
        out_shape=(jax.ShapeDtypeStruct(pressure.shape, jnp.float32),) * 2,
        in_specs=[vmem_space, vmem_space],
        out_specs=(any_space, any_space),
        scratch_shapes=[pltpu.VMEM(pressure.shape, jnp.float32), dma, dma],
        compiler_params=pltpu.CompilerParams(vmem_limit_bytes=24 * 1024 * 1024),
    )(end, stat)


def solution(mesh):
    spec = P("rows", "cols", "slabs", None)
    sizes = tuple(mesh.shape[name] for name in ("rows", "cols", "slabs"))
    return jax.shard_map(functools.partial(shards, sizes), mesh=mesh,
                         in_specs=(spec,) * 3, out_specs=(spec,) * 2, check_vma=False)
```

```python
import functools

import jax
import jax.numpy as jnp
from jax import lax
from jax.experimental import pallas as pl
from jax.experimental.pallas import tpu as pltpu
from jax.sharding import PartitionSpec as P

STEPS = 3
GUESS = 1.0
EPS = 0.0001
MESH = pl.DeviceIdType.MESH
TILE = 8
PARTS = 8
LO, HI = 0, 1


def halving(planes):
    spans, start = [], 0
    while planes - start > TILE:
        size = (planes - start) // (2 * TILE) * TILE
        spans.append((start, size))
        start += size
    return spans + [(start, planes - start)]


def leapfrog(sizes, p_hbm, e_hbm, s_hbm, end, stat,
             even, odd, xh, yh, line,
             xs, xr, xp, ys, yr, zs, zr, ls, lr, own, heard):
    speed = end
    rows, cols, slabs = sizes
    planes, cells, depth = p_hbm.shape[0], p_hbm.shape[1], p_hbm.shape[2]
    tiles = depth // TILE
    body_planes = pl.ds(1, planes)
    row, col, slab = (lax.axis_index(name) for name in ("rows", "cols", "slabs"))

    def shifted(name, index, count, by):
        return {name: lax.rem(index + by + count, count)}

    x_to = (shifted("cols", col, cols, -1), shifted("cols", col, cols, 1))
    y_to = (shifted("slabs", slab, slabs, -1), shifted("slabs", slab, slabs, 1))
    z_to = (shifted("rows", row, rows, -1), shifted("rows", row, rows, 1))
    peers = [shifted("rows", row, rows, d) for d in range(1, rows)]

    loads = [
        pltpu.make_async_copy(p_hbm, even.at[body_planes], own.at[0]),
        pltpu.make_async_copy(e_hbm, odd.at[body_planes], own.at[1]),
        pltpu.make_async_copy(s_hbm, speed, own.at[2]),
    ]
    barrier = pltpu.get_barrier_semaphore()
    near = y_to + z_to

    def greet(devices):
        for device in devices:
            pl.semaphore_signal(barrier, inc=1, device_id=device, device_id_type=MESH)

    paired = slabs % 2 == 0
    early = lax.rem(slab, 2) == 0
    greet(x_to)
    if paired:
        pl.when(jnp.logical_not(early))(lambda: greet(z_to))
        pl.semaphore_wait(barrier, len(x_to) + len(near) * lax.rem(slab, 2))
        greet(y_to)
    else:
        greet(near)
        pl.semaphore_wait(barrier, len(x_to) + len(near))

    fields = (even, odd)
    count = float(planes * rows)

    def order(step):
        return (LO, HI) if step % 2 == 0 else (HI, LO)

    def edge_cell(side):
        return 0 if side == LO else cells - 1

    sooner, later = (edge_cell(1 - side) for side in order(STEPS - 1))
    groups = [
        (pl.ds(1, cells - 2), slice(None), [(c, q) for c in range(1, cells - 1) for q in range(tiles)]),
        (sooner, slice(None), [(sooner, q) for q in range(tiles)]),
        (later, pl.ds(0, tiles - 1), [(later, q) for q in range(tiles - 1)]),
        (later, tiles - 1, [(later, tiles - 1)]),
    ]

    def line_copy(group, d):
        part = line.at[row, groups[group][0], groups[group][1]]
        return remote(part, part, ls.at[d], lr.at[group, d], peers[d])

    def send_lines(group):
        for d in range(rows - 1):
            if group > 0:
                line_copy(group - 1, d).wait_send()
            line_copy(group, d).start()

    def remote(src, dst, send, recv, device):
        return pltpu.make_async_remote_copy(
            src_ref=src, dst_ref=dst, send_sem=send, recv_sem=recv,
            device_id=device, device_id_type=MESH,
        )

    def source(step):
        return p_hbm if step == 0 else fields[step % 2].at[body_planes]

    def x_part(step, side, here, part, recv):
        return remote(source(step).at[here, edge_cell(side), part, :], xh.at[step, 1 - side, here, part, :],
                      xs.at[step % 2, side], recv, x_to[side])

    def x_copies(step, side, q):
        part = pl.ds(q * TILE, TILE)
        if step == STEPS - 1 and side == order(step)[1] and q == tiles - 1:
            return [x_part(step, side, pl.ds(*span), part, xp.at[i]) for i, span in enumerate(halving(planes))]
        return [x_part(step, side, slice(None), part, xr.at[step % 2, side, q])]

    def x_sent(step, side):
        x_part(step, side, slice(None), slice(None), xp.at[0]).wait_send()

    def y_copy(step, side):
        part = pl.ds(0 if side == LO else depth - TILE, TILE)
        return remote(source(step).at[:, :, part, :], yh.at[step, 1 - side],
                      ys.at[side], yr.at[step % 2, side], y_to[side])

    def z_copy(step, side):
        src = p_hbm.at[0 if side == LO else planes - 1] if step == 0 else (
            fields[step % 2].at[1 if side == LO else planes])
        dst = fields[step % 2].at[planes + 1 if side == LO else 0]
        return remote(src, dst, zs.at[side], zr.at[step % 2, side], z_to[side])

    def update(step, cell, q, low, high, copies=(), before_last=None):
        now, then = fields[step % 2], fields[(step + 1) % 2]
        part = pl.ds(q * TILE, TILE)
        index = lax.broadcasted_iota(jnp.int32, (TILE, TILE, 128), 1)
        last = step == STEPS - 1

        def block(b, sums):
            j = b * TILE
            here, padded = pl.ds(j, TILE), pl.ds(j + 1, TILE)
            mid = now[padded, cell, part, :]
            if q == 0:
                below = yh[step, LO, here, cell, TILE - 1:TILE, :]
            else:
                below = now[padded, cell, q * TILE - 1:q * TILE, :]
            if q == tiles - 1:
                above = yh[step, HI, here, cell, 0:1, :]
            else:
                above = now[padded, cell, (q + 1) * TILE:(q + 1) * TILE + 1, :]
            k_low = jnp.where(index == 0, below, pltpu.roll(mid, 1, 1))
            k_high = jnp.where(index == TILE - 1, above, pltpu.roll(mid, TILE - 1, 1))
            spread = (now[here, cell, part, :] + now[pl.ds(j + 2, TILE), cell, part, :]
                      + low(here, padded, part) + high(here, padded, part)
                      + k_low + k_high - 6.0 * mid)
            new = 2.0 * mid - then[padded, cell, part, :] + speed[here, cell, part, :] * spread
            if last:
                end[here, cell, part, :] = new
                moved = new - GUESS
                return sums[0] + jnp.sum(moved, axis=0), sums[1] + jnp.sum(moved * moved, axis=0)
            then[padded, cell, part, :] = new
            return sums

        zero = jnp.zeros((TILE, 128), jnp.float32)
        sums = (zero, zero) if last else 0
        spans = halving(planes) if len(copies) > 1 else [(0, planes)]
        for i, (start, size) in enumerate(spans):
            if before_last is not None and i == len(spans) - 1:
                before_last()
            if copies:
                copies[i].wait_recv()
            sums = lax.fori_loop(start // TILE, (start + size) // TILE, block, sums)
        if last:
            line[row, cell, q, 0] = sums[0]
            line[row, cell, q, 1] = sums[1]

    def edge(step, side, q, copies, before_last):
        now = fields[step % 2]
        halo = lambda here, padded, part: xh[step, side, here, part, :]
        if side == LO:
            update(step, 0, q, halo, lambda here, padded, part: now[padded, 1, part, :], copies, before_last)
        else:
            update(step, cells - 1, q, lambda here, padded, part: now[padded, cells - 2, part, :], halo, copies, before_last)

    def interior(step):
        now = fields[step % 2]

        def at(cell, carry):
            for q in range(tiles):
                update(step, cell, q,
                       lambda here, padded, part: now[padded, cell - 1, part, :],
                       lambda here, padded, part: now[padded, cell + 1, part, :])
            return carry

        lax.fori_loop(1, cells - 1, at, 0)

    def settle(group):
        for d in range(rows - 1):
            line_copy(group, d).wait_recv()
        for cell, q in groups[group][2]:
            total, square = line[0, cell, q, 0], line[0, cell, q, 1]
            for r in range(1, rows):
                total, square = total + line[r, cell, q, 0], square + line[r, cell, q, 1]
            shift = total / count
            part = pl.ds(q * TILE, TILE)
            stat[0, cell, part, :] = GUESS + shift
            stat[1, cell, part, :] = lax.rsqrt(square / count - shift * shift + EPS)

    def start_cols():
        for side in order(0):
            for q in range(tiles):
                for copy in x_copies(0, side, q):
                    copy.start()

    if paired:
        pl.when(early)(start_cols)
    else:
        start_cols()
    def swap_rows():
        for side in (LO, HI):
            z_copy(0, side).start()
        for side in (LO, HI):
            z_copy(0, side).wait_recv()

    def start_early():
        pl.semaphore_wait(barrier, len(y_to))
        for side in (LO, HI):
            y_copy(0, side).start()
        pl.semaphore_wait(heard, len(y_to))
        swap_rows()

    def start_late():
        for side in (LO, HI):
            y_copy(0, side).start()
        swap_rows()
        start_cols()
        for device in y_to:
            pl.semaphore_signal(heard, inc=1, device_id=device, device_id_type=MESH)

    for load in loads:
        load.start()
    if paired:
        pl.when(early)(start_early)
        pl.when(jnp.logical_not(early))(start_late)
    else:
        for side in (LO, HI):
            y_copy(0, side).start()
        swap_rows()
    for load in loads:
        load.wait()

    for step in range(STEPS):
        if step >= 1:
            for side in order(step - 1):
                z_copy(step - 1, side).wait_send()
                y_copy(step - 1, side).wait_send()
                x_sent(step - 1, side)
        for side in (LO, HI):
            if step >= 1:
                z_copy(step, side).wait_recv()
            y_copy(step, side).wait_recv()
        interior(step)
        if step == STEPS - 1:
            send_lines(0)
        first, second = order(step)
        for side in (first, second):
            for q in range(tiles):
                final = step == STEPS - 1
                hook = functools.partial(settle, 2) if final and side == second and q == tiles - 1 else None
                edge(step, 1 - side, q, x_copies(step, side, q), hook)
                if not final:
                    for copy in x_copies(step + 1, 1 - side, q):
                        copy.start()
                elif side == first:
                    if q == 0:
                        settle(0)
                    if q == tiles - 1:
                        send_lines(1)
                else:
                    if q == 0:
                        settle(1)
                    if q >= tiles - 2:
                        send_lines(q - tiles + 4)
        if step < STEPS - 1:
            for side in (LO, HI):
                z_copy(step + 1, side).start()
                y_copy(step + 1, side).start()

    for side in order(STEPS - 1):
        z_copy(STEPS - 1, side).wait_send()
        y_copy(STEPS - 1, side).wait_send()
        x_sent(STEPS - 1, side)

    settle(3)
    for d in range(rows - 1):
        line_copy(3, d).wait_send()


def rescale(p_ref, stat_ref, scaled_hbm, end_hbm, scaled, end_sem, scaled_sem):
    planes = p_ref.shape[0]
    each = planes // PARTS
    parts = [pl.ds(c * each, each) for c in range(PARTS)]
    for part in parts:
        pltpu.make_async_copy(p_ref.at[part], end_hbm.at[part], end_sem).start()

    def plane(j, carry):
        scaled[j] = (p_ref[j] - stat_ref[0]) * stat_ref[1]
        return carry

    for c, part in enumerate(parts):
        lax.fori_loop(c * each, (c + 1) * each, plane, 0, unroll=2)
        pltpu.make_async_copy(scaled.at[part], scaled_hbm.at[part], scaled_sem).start()
    pltpu.make_async_copy(p_ref, end_hbm, end_sem).wait()
    pltpu.make_async_copy(scaled, scaled_hbm, scaled_sem).wait()


def shards(sizes, pressure, earlier, speed_square):
    rows = sizes[0]
    planes, cells, depth, members = pressure.shape
    tiles = depth // TILE
    any_space = pl.BlockSpec(memory_space=pl.ANY)
    dma = pltpu.SemaphoreType.DMA
    vmem_space = pl.BlockSpec(memory_space=pltpu.VMEM)
    end, stat = pl.pallas_call(
        functools.partial(leapfrog, sizes),
        out_shape=(
            pltpu.VMEM(pressure.shape, jnp.float32),
            pltpu.VMEM((2, cells, depth, members), jnp.float32),
        ),
        in_specs=[any_space] * 3,
        out_specs=(vmem_space, vmem_space),
        scratch_shapes=[
            pltpu.VMEM((planes + 2, cells, depth, members), jnp.float32),
            pltpu.VMEM((planes + 2, cells, depth, members), jnp.float32),
            pltpu.VMEM((STEPS, 2, planes, depth, members), jnp.float32),
            pltpu.VMEM((STEPS, 2, planes, cells, TILE, members), jnp.float32),
            pltpu.VMEM((rows, cells, tiles, 2, TILE, members), jnp.float32),
            dma((2, 2)), dma((2, 2, tiles)), dma((len(halving(planes)),)),
            dma((2,)), dma((2, 2)),
            dma((2,)), dma((2, 2)),
            dma((rows - 1,)), dma((4, rows - 1)),
            dma((3,)),
            pltpu.SemaphoreType.REGULAR,
        ],
        compiler_params=pltpu.CompilerParams(
            collective_id=0, has_side_effects=True, vmem_limit_bytes=46 * 1024 * 1024
        ),
    )(pressure, earlier, speed_square)

    return pl.pallas_call(
        rescale,
        out_shape=(jax.ShapeDtypeStruct(pressure.shape, jnp.float32),) * 2,
        in_specs=[vmem_space, vmem_space],
        out_specs=(any_space, any_space),
        scratch_shapes=[pltpu.VMEM(pressure.shape, jnp.float32), dma, dma],
        compiler_params=pltpu.CompilerParams(vmem_limit_bytes=24 * 1024 * 1024),
    )(end, stat)


def solution(mesh):
    spec = P("rows", "cols", "slabs", None)
    sizes = tuple(mesh.shape[name] for name in ("rows", "cols", "slabs"))
    return jax.shard_map(functools.partial(shards, sizes), mesh=mesh,
                         in_specs=(spec,) * 3, out_specs=(spec,) * 2, check_vma=False)
```
